32 devices in a mesh: gx: 4 (over x, core), gy: 4 (over z), gz: 2 (over y).
Axes of the slice: x: 2, y: 2, z: 4, core: 2. Of those that a mesh axis runs over, the one named last changes fastest.
Arguments:
- particle_fields: float32 [20, 262144], P(None, ('gx', 'gy', 'gz')), may hold values from -4 to 4
- step_length: float32 [262144], P(('gx', 'gy', 'gz')), may hold values from 0.1 to 1
- live_mask: int32 [262144], P(('gx', 'gy', 'gz')), may hold values 0 or 1
- dest_cell: int32 [262144], P(('gx', 'gy', 'gz')), may hold values from 0 to 511
- block_counts: int32 [32, 6], P(('gx', 'gy', 'gz')), may hold values from 0 to 12, as said below
- block_lists: int32 [32, 48], P(('gx', 'gy', 'gz')), may hold values from 0 to 87, as said below
Outputs:
- tile_sums: float32 [20, 16384], P(None, ('gx', 'gy', 'gz'))
The draws below stay inside these ranges and needn't reach their ends.
Inputs may be any that keep to these rules, and one draw needn't show every extreme that they name: `block_counts`: columns are directions in the order x lower, x upper, z lower, z upper, y lower, y upper; a count is at most its section's span (6, 6 or 12) and may be 0; at every section some domain receives full spans from both neighbours. `block_lists`: per domain, 6 entries toward the lower x neighbour, 6 toward the upper, then 2 * 6 for z and 24 for y in the same way; entries are block numbers of the domain's pool at that section. Entries below their direction's count are valid: valid entries of one domain over all sections are distinct, and each names an own block or an appended block that its sender filled. Other entries are arbitrary numbers within the pool.
All inputs are finite; a program needn't handle non-finite values. No bound on the sum of `live_mask` on one device may be relied on, other than what follows from the above.
Results may differ from the reference program's by a relative error of at most 0.0003.
Values sent between devices are 32-bit elements; how exact they have to be, the bound alone decides.
No kernel may reach another device: no remote copies, remote signals or barrier semaphores. Data moves between devices by JAX's collectives and lax.ppermute only.
A program may use at most 64 MiB of HBM per device.

```python
import math
import jax
import jax.numpy as jnp

FIELDS = 20
BLOCKS = 64
CELLS = 512
CAP_X = 6
CAP_Z = 6
CAP_Y = 12
LIST_LEN = 48
PARTICLES = 262144
N_GX = 4
N_GY = 4
N_GZ = 2


def plan_migration(key):
    shape_grid = (N_GX, N_GY, N_GZ)
    final_count = BLOCKS + 2 * (CAP_X + CAP_Z + CAP_Y)
    pool_index = jnp.arange(final_count, dtype=jnp.int32)
    eligible = jnp.broadcast_to(pool_index < BLOCKS, shape_grid + (final_count,))
    coords = jnp.meshgrid(jnp.arange(N_GX, dtype=jnp.int32), jnp.arange(N_GY, dtype=jnp.int32), jnp.arange(N_GZ, dtype=jnp.int32), indexing='ij')
    extents_grid = jnp.array(shape_grid, dtype=jnp.int32)
    size_now = BLOCKS
    count_parts = []
    list_parts = []
    for section_index, (axis_place, extent) in enumerate(((0, CAP_X), (2, CAP_Z), (1, CAP_Y))):
        section_key = jax.random.fold_in(key, 101 + section_index)
        count_key, pick_key, filler_key, target_key = jax.random.split(section_key, 4)
        rough_draw = jax.random.randint(count_key, shape_grid + (2,), 0, extent + 1, dtype=jnp.int32)
        number = rough_draw * rough_draw // extent
        target = jax.random.randint(target_key, (3,), 0, extents_grid, dtype=jnp.int32)
        step_unit = (jnp.arange(3) == axis_place).astype(jnp.int32)
        lower_site = (target - step_unit) % extents_grid
        upper_site = (target + step_unit) % extents_grid
        at_lower = (coords[0] == lower_site[0]) & (coords[1] == lower_site[1]) & (coords[2] == lower_site[2])
        at_upper = (coords[0] == upper_site[0]) & (coords[1] == upper_site[1]) & (coords[2] == upper_site[2])
        toward_lower = jnp.where(at_upper, extent, number[..., 0]).astype(jnp.int32)
        toward_upper = jnp.where(at_lower, extent, number[..., 1]).astype(jnp.int32)
        scores = jax.random.randint(pick_key, shape_grid + (final_count,), 0, 1 << 20, dtype=jnp.int32) * final_count + pool_index
        scores = jnp.where(eligible, scores, -1)
        chosen = jnp.argsort(-scores, axis=-1)[..., :2 * extent].astype(jnp.int32)
        position = jnp.arange(2 * extent) % extent
        wanted = jnp.where(jnp.arange(2 * extent) < extent, toward_lower[..., None], toward_upper[..., None])
        usable = position < wanted
        filler = jax.random.randint(filler_key, shape_grid + (2 * extent,), 0, size_now, dtype=jnp.int32)
        list_parts.append(jnp.where(usable, chosen, filler))
        count_parts.append(jnp.stack([toward_lower, toward_upper], axis=-1))
        taken_now = jnp.any((chosen[..., :, None] == pool_index) & usable[..., None], axis=-2)
        from_lower = jnp.roll(toward_upper, 1, axis=axis_place)
        from_upper = jnp.roll(toward_lower, -1, axis=axis_place)
        offset = pool_index - size_now
        landed = (offset >= 0) & (offset < extent) & (offset < from_lower[..., None]) | (offset >= extent) & (offset < 2 * extent) & (offset - extent < from_upper[..., None])
        eligible = eligible & jnp.logical_not(taken_now) | landed
        size_now = size_now + 2 * extent
    counts = jnp.concatenate(count_parts, axis=-1).reshape(N_GX * N_GY * N_GZ, 6)
    entries = jnp.concatenate(list_parts, axis=-1).reshape(N_GX * N_GY * N_GZ, 2 * (CAP_X + CAP_Z + CAP_Y))
    return (counts.astype(jnp.int32), entries.astype(jnp.int32))


def draw_block_counts(key, part):
    return plan_migration(key)[0]


def draw_block_lists(key, part):
    return plan_migration(key)[1]


def set_ends(values, stream_key, low, high):
    dims = values.shape
    place = [jax.random.randint(jax.random.fold_in(stream_key, axis), (), 0, dims[axis]) for axis in range(len(dims))]
    values = values.at[tuple(place)].set(low)
    longest = dims.index(max(dims))
    place[longest] = (place[longest] + 1) % dims[longest]
    return values.at[tuple(place)].set(high)


def levels(stream_key, dims, pieces, least, high):
    loudness, own = 1.0, jax.random.fold_in(stream_key, 6)
    for axis_at, shards_of in pieces:
        steps = jnp.exp(jax.random.uniform(jax.random.fold_in(own, axis_at), (shards_of,), jnp.float32, least / len(pieces), high / len(pieces)))
        loudness = loudness * jnp.repeat(steps, dims[axis_at] // shards_of).reshape([-1 if axis == axis_at else 1 for axis in range(len(dims))])
    return loudness


def centred(rng, shape, deviation, reach, cuts=(), kind=jnp.bfloat16):
    values = jax.random.normal(rng, shape, jnp.float32) * deviation
    if len(cuts) > 0:
        values = levels(rng, shape, cuts, -0.22, 0.18) * values
    return jnp.clip(values, min=-reach, max=reach).astype(kind)


def setup_inputs(seed: int = 0) -> dict:
    arg_keys = jax.random.split(jax.random.key(seed), 7)
    return {
        "particle_fields": centred(arg_keys[0], (FIELDS, PARTICLES), 0.25, 4.0, ((1, 32),), jnp.float32),
        "step_length": jnp.clip(jnp.exp(math.log(1.0) - 2.3025851 * jax.random.uniform(arg_keys[1], (PARTICLES,), jnp.float32) ** levels(arg_keys[1], (PARTICLES,), ((0, 32),), -0.2, 0.2)), 0.1, 1.0),
        "live_mask": set_ends((jax.random.randint(arg_keys[2], (PARTICLES,), 0, 4) < 3).astype(jnp.int32), jax.random.fold_in(arg_keys[2], 1), 0, 1),
        "dest_cell": set_ends(jax.random.randint(arg_keys[3], (PARTICLES,), 0, CELLS), jax.random.fold_in(arg_keys[3], 1), 0, CELLS - 1).astype(jnp.int32),
        "block_counts": draw_block_counts(jax.random.fold_in(arg_keys[6], 71), 0),
        "block_lists": draw_block_lists(jax.random.fold_in(arg_keys[6], 71), 0),
    }


def leave_section(holding, chosen, number, axis_place):
    extent = chosen.shape[-1] // 2
    index_full = jnp.broadcast_to(chosen.astype(jnp.int32)[None, :, :, :, :, None], holding.shape[:4] + (2 * extent, 128))
    picked = jnp.take_along_axis(holding, index_full, axis=4)
    position = jnp.arange(2 * extent) % extent
    wanted = jnp.where(jnp.arange(2 * extent) < extent, number[..., 0:1], number[..., 1:2])
    usable = (position < wanted).astype(jnp.float32)
    outgoing = picked * usable[None, :, :, :, :, None]
    from_lower = jnp.roll(outgoing[:, :, :, :, extent:], 1, axis=axis_place + 1)
    from_upper = jnp.roll(outgoing[:, :, :, :, :extent], -1, axis=axis_place + 1)
    return jnp.concatenate([holding, from_lower, from_upper], axis=4)


def reference(particle_fields, step_length, live_mask, dest_cell, block_counts, block_lists):
    advanced = particle_fields[0:3] + step_length[None, :] * particle_fields[3:6]
    carried = jnp.concatenate([advanced, particle_fields[3:], live_mask.astype(jnp.float32)[None, :], dest_cell.astype(jnp.float32)[None, :]], axis=0)
    row_count = FIELDS + 2
    domain_count = N_GX * N_GY * N_GZ
    holding = carried.reshape(row_count, N_GX, N_GY, N_GZ, BLOCKS, 128)
    number = block_counts.reshape(N_GX, N_GY, N_GZ, 6)
    entries = block_lists.reshape(N_GX, N_GY, N_GZ, LIST_LEN)
    first_end = 2 * CAP_X
    second_end = first_end + 2 * CAP_Z
    holding = leave_section(holding, entries[..., :first_end], number[..., 0:2], 0)
    holding = leave_section(holding, entries[..., first_end:second_end], number[..., 2:4], 2)
    before_count = holding.shape[4]
    holding = leave_section(holding, entries[..., second_end:], number[..., 4:6], 1)
    spans = (CAP_X, CAP_X, CAP_Z, CAP_Z, CAP_Y, CAP_Y)
    limits = [jnp.broadcast_to(number[..., column:column + 1], (N_GX, N_GY, N_GZ, extent)) for column, extent in enumerate(spans)]
    wanted = jnp.concatenate(limits, axis=-1)
    position = jnp.concatenate([jnp.arange(extent) for extent in spans])
    listed = (entries[..., :, None] == jnp.arange(before_count)[None, None, None, None, :]) & (position < wanted)[..., None]
    keep_before = 1.0 - jnp.any(listed, axis=3).astype(jnp.float32)
    keep_block = jnp.concatenate([keep_before, jnp.ones((N_GX, N_GY, N_GZ, holding.shape[4] - before_count), jnp.float32)], axis=-1)
    weights = holding[FIELDS] * keep_block[..., None]
    domain = jnp.arange(domain_count, dtype=jnp.int32).reshape(N_GX, N_GY, N_GZ, 1, 1)
    segment = (domain * CELLS + holding[FIELDS + 1].astype(jnp.int32)).reshape(-1)
    columns = []
    for field_index in range(FIELDS):
        columns.append(jax.ops.segment_sum((holding[field_index] * weights).reshape(-1), segment, num_segments=domain_count * CELLS))
    return jnp.stack(columns, axis=0)
```

```python
import jax
import jax.numpy as jnp
from jax import lax
from jax.experimental import pallas as pl
from jax.experimental.pallas import tpu as pltpu
from jax.sharding import PartitionSpec as P

CELLS = 512
CAP_X = 6
CAP_Z = 6
CAP_Y = 12
LANES = 128
SLAB = 24
GROUPS = CELLS // LANES
F32 = jnp.float32
BF16 = jnp.bfloat16

VMEM = pl.BlockSpec(memory_space=pltpu.VMEM)
SMEM = pl.BlockSpec(memory_space=pltpu.SMEM)


def params(mib):
    return pltpu.CompilerParams(vmem_limit_bytes=mib << 20)


def cost(flops, nbytes):
    return pl.CostEstimate(flops=flops, bytes_accessed=nbytes, transcendentals=0)


def pairwise(n):
    return n > 2 and n % 2 == 0


def flip_of(axis):
    return lax.axis_index(axis) % 2 if pairwise(lax.axis_size(axis)) else 0


def swapped_of(axis):
    return lax.axis_index(axis) % 2 if pairwise(lax.axis_size(axis)) else 1


def exchange(axis, bufs):
    n = lax.axis_size(axis)
    if n == 2:
        return [lax.ppermute(bufs[0], axis, [(0, 1), (1, 0)])]
    if pairwise(n):
        first = [(i, (i + 1) % n if i % 2 else (i - 1) % n) for i in range(n)]
        second = [(i, (i - 1) % n if i % 2 else (i + 1) % n) for i in range(n)]
    else:
        first = [(i, (i - 1) % n) for i in range(n)]
        second = [(i, (i + 1) % n) for i in range(n)]
    return [lax.ppermute(bufs[0], axis, first), lax.ppermute(bufs[1], axis, second)]


def buffer_shapes(axis, rows):
    n = lax.axis_size(axis)
    one = jax.ShapeDtypeStruct((2 * rows if n == 2 else rows, LANES), F32)
    return [one] if n == 2 else [one, one]


def half(refs, side, rows):
    if len(refs) == 1:
        return refs[0], side * rows
    return refs[side], 0


def packed_rows(fields, count):
    return -(-(count * (fields + 1)) // 8) * 8


def put_block(ref, base, slot, count, fields, slab):
    ref[pl.ds(base + slot * fields, fields), :] = slab[:fields]
    ref[pl.ds(base + count * fields + slot, 1), :] = slab[fields : fields + 1]


def get_block(ref, base, slot, count, fields):
    body = ref[pl.ds(base + slot * fields, fields), :]
    cell = ref[pl.ds(base + count * fields + slot, 1), :]
    pad = jnp.zeros((SLAB - fields - 1, LANES), F32)
    return jnp.concatenate([body, cell, pad], axis=0)


def drifted(fields_ref, step_ref, live_ref, cell_ref, block):
    lanes = pl.ds(pl.multiple_of(block * LANES, LANES), LANES)
    fields = fields_ref.shape[0]
    top = fields_ref[0:8, lanes]
    step = step_ref[pl.ds(block, 1), :]
    live = live_ref[pl.ds(block, 1), :].astype(F32)
    cell = cell_ref[pl.ds(block, 1), :].astype(F32)
    row = lax.broadcasted_iota(jnp.int32, (8, LANES), 0)
    top = top + jnp.where(row < 3, pltpu.roll(top, 5, 0) * step, 0.0)
    rest = fields_ref[8:fields, lanes]
    pad = jnp.zeros((SLAB - fields - 1, LANES), F32)
    return jnp.concatenate([top * live, rest * live, cell, pad], axis=0)


def binned(slabs):
    left, right = [], []
    lane_cell = lax.broadcasted_iota(jnp.int32, (LANES, LANES), 0)
    for slab, field in slabs:
        cell = slab[field : field + 1].astype(jnp.int32)
        low, group = cell & (LANES - 1), cell >> 7
        right.append(jnp.where(lane_cell == low, 1.0, 0.0).astype(BF16))
        high = slab.astype(BF16).astype(F32)
        both = jnp.concatenate([high, slab - high], axis=0)
        left.append(
            jnp.concatenate(
                [jnp.where(group == g, both, 0.0).astype(BF16) for g in range(GROUPS)], axis=0
            )
        )
    return lax.dot_general(
        jnp.concatenate(left, axis=1),
        jnp.concatenate(right, axis=1),
        (((1,), (1,)), ((), ())),
        preferred_element_type=F32,
    )


ACC = (GROUPS * 2 * SLAB, LANES)


def put_sums(ref, base, acc, fields):
    for g in range(GROUPS):
        top = 2 * SLAB * g
        ref[pl.ds(base + g * fields, fields), :] = (
            acc[top : top + fields] + acc[top + SLAB : top + SLAB + fields]
        )


def x_out_kernel(axis, fields, number, entries, f_ref, s_ref, l_ref, c_ref, *outs):
    flip = flip_of(axis)
    rows = packed_rows(fields, CAP_X)
    for side in range(2):
        way = flip if side == 0 else 1 - flip
        ref, base = half(outs, side, rows)
        for j in range(CAP_X):
            entry = entries[0, way * CAP_X + j]
            entry = jnp.where(j < number[0, way], entry, 0)
            slab = drifted(f_ref, s_ref, l_ref, c_ref, entry)
            put_block(ref, base, j, CAP_X, fields, slab * (j < number[0, way]).astype(F32))
        used = CAP_X * (fields + 1)
        if rows > used:
            ref[pl.ds(base + used, rows - used), :] = jnp.zeros((rows - used, LANES), F32)


def arrival_place(entry, first, cap, swapped):
    place = entry - first + cap * swapped
    return jnp.where(place >= 2 * cap, place - 2 * cap, place)


def pool_kernel(axes, fields, blocks, number, entries, f_ref, s_ref, l_ref, c_ref, pool, z_own, z_pick):
    x_axis, z_axis = axes

    @pl.loop(0, blocks, unroll=4)
    def _(b):
        pool[b] = drifted(f_ref, s_ref, l_ref, c_ref, b)

    flip = flip_of(z_axis)
    swapped = swapped_of(x_axis)
    for side in range(2):
        way = flip if side == 0 else 1 - flip
        for j in range(CAP_Z):
            slot = side * CAP_Z + j
            valid = j < number[0, 2 + way]
            entry = entries[0, 2 * CAP_X + way * CAP_Z + j]
            own = valid & (entry < blocks)
            z_own[slot] = pool[jnp.where(own, entry, 0)] * own.astype(F32)
            place = arrival_place(entry, blocks, CAP_X, swapped)
            place = jnp.where(valid & (entry >= blocks), place, -1)
            row = lax.broadcasted_iota(jnp.int32, (16, LANES), 0)
            z_pick[slot] = (row == place).astype(F32)


def make_z_out(fields, n_in):
    x_rows = packed_rows(fields, CAP_X)
    z_rows = packed_rows(fields, CAP_Z)

    def kernel(z_own, z_pick, *refs):
        arrivals, outs = refs[:n_in], refs[n_in:]
        came = []
        for place in range(2 * CAP_X):
            ref, base = half(arrivals, place // CAP_X, x_rows)
            came.append(get_block(ref, base, place % CAP_X, CAP_X, fields))
        for side in range(2):
            ref, base = half(outs, side, z_rows)
            for j in range(CAP_Z):
                slot = side * CAP_Z + j
                slab = z_own[slot]
                for place in range(2 * CAP_X):
                    slab = slab + came[place] * z_pick[slot, place : place + 1, :]
                put_block(ref, base, j, CAP_Z, fields, slab)
            used = CAP_Z * (fields + 1)
            if z_rows > used:
                ref[pl.ds(base + used, z_rows - used), :] = jnp.zeros((z_rows - used, LANES), F32)

    return kernel


def make_bin(fields, blocks, axes, n_in):
    x_axis, z_axis, y_axis = axes
    x_rows = packed_rows(fields, CAP_X)
    held = blocks + 2 * CAP_X
    total = held + 2 * CAP_Z

    def kernel(number, entries, pool, *refs):
        arrivals = refs[:n_in]
        stay, y_part, z_mask, codes, x_pool, y_acc = refs[n_in:]
        x_swapped, z_swapped, y_flip = swapped_of(x_axis), swapped_of(z_axis), flip_of(y_axis)
        for place in range(2 * CAP_X):
            ref, base = half(arrivals, place // CAP_X, x_rows)
            x_pool[place] = get_block(ref, base, place % CAP_X, CAP_X, fields)

        for b in range(total + 1):
            codes[b] = 0

        def spot(entry):
            in_x = arrival_place(entry, blocks, CAP_X, x_swapped) + blocks
            in_z = arrival_place(entry, held, CAP_Z, z_swapped) + held
            return jnp.where(entry < blocks, entry, jnp.where(entry < held, in_x, in_z))

        at = 0
        for section, cap in enumerate((CAP_X, CAP_Z, CAP_Y)):
            for way in range(2):
                for j in range(cap):
                    valid = j < number[0, 2 * section + way]
                    code = 1 if section < 2 else 2 + (way if isinstance(y_flip, int) else way ^ y_flip)
                    codes[jnp.where(valid, spot(entries[0, at]), total)] = code
                    at += 1

        for b in range(2 * CAP_Z):
            code = codes[held + b]
            for k in range(3):
                wanted = (0, 2, 3)[k]
                z_mask[k, b : b + 1, :] = jnp.full((1, LANES), (code == wanted).astype(F32))

        first = 2 * CAP_X + 2 * CAP_Z
        for side in range(2):
            way = side if isinstance(y_flip, int) else side ^ y_flip

            def one(j):
                entry = spot(entries[0, first + way * CAP_Y + j])
                valid = (j < number[0, 4 + way]) & (entry < held)
                own = valid & (entry < blocks)
                mine = pool[jnp.where(own, entry, 0)] * own.astype(F32)
                theirs = valid & (entry >= blocks)
                return mine + x_pool[jnp.where(theirs, entry - blocks, 0)] * theirs.astype(F32)

            acc = jnp.zeros(ACC, F32)
            for j in range(0, CAP_Y, 4):
                acc = acc + binned([(one(j + i), fields) for i in range(4)])
            y_part[side] = acc

        y_acc[...] = jnp.zeros(ACC, F32)

        @pl.loop(0, blocks // 8)
        def _(step):
            slabs = []
            for i in range(8):
                b = step * 8 + i
                slabs.append((keep_block(pool[b], codes[b] == 0, fields), fields))
            y_acc[...] += binned(slabs)

        acc = y_acc[...]
        for p in range(0, 2 * CAP_X, 6):
            slabs = []
            for i in range(6):
                slabs.append((keep_block(x_pool[p + i], codes[blocks + p + i] == 0, fields), fields))
            acc = acc + binned(slabs)
        stay[...] = acc

    return kernel


def keep_block(slab, keep, fields):
    row = lax.broadcasted_iota(jnp.int32, (SLAB, LANES), 0)
    return slab * jnp.where(row == fields, 1.0, keep.astype(F32))


def z_slab(arrivals, mask, kind, place, rows, fields):
    ref, base = half(arrivals, place // CAP_Z, rows)
    body = ref[pl.ds(base + (place % CAP_Z) * fields, fields), :] * mask[kind, place : place + 1, :]
    cell = ref[pl.ds(base + CAP_Z * fields + place % CAP_Z, 1), :]
    pad = jnp.zeros((SLAB - fields - 1, LANES), F32)
    return jnp.concatenate([body, cell, pad], axis=0)


def make_y_out(fields, n_in):
    rows = packed_rows(fields, CAP_Z)

    def kernel(y_part, z_mask, *refs):
        arrivals, outs = refs[:n_in], refs[n_in:]
        for side in range(2):
            slabs = [
                (z_slab(arrivals, z_mask, 1 + side, place, rows, fields), fields)
                for place in range(2 * CAP_Z)
            ]
            ref, base = half(outs, side, GROUPS * fields)
            put_sums(ref, base, y_part[side] + binned(slabs), fields)

    return kernel


def make_stay(fields, n_in):
    rows = packed_rows(fields, CAP_Z)

    def kernel(stay, z_mask, *refs):
        arrivals, out = refs[:n_in], refs[n_in]
        slabs = [
            (z_slab(arrivals, z_mask, 0, place, rows, fields), fields) for place in range(2 * CAP_Z)
        ]
        put_sums(out, 0, stay[...] + binned(slabs), fields)

    return kernel


def make_final(fields, n_in):
    def kernel(stay, *refs):
        arrivals, out = refs[:n_in], refs[n_in]
        for g in range(GROUPS):
            total = stay[g * fields : (g + 1) * fields, :]
            for side in range(2):
                ref, base = half(arrivals, side, GROUPS * fields)
                total = total + ref[pl.ds(base + g * fields, fields), :]
            out[:, g * LANES : (g + 1) * LANES] = total

    return kernel


def per_device(particle_fields, step_length, live_mask, dest_cell, block_counts, block_lists):
    fields = particle_fields.shape[0]
    blocks = particle_fields.shape[1] // LANES
    data = (
        particle_fields,
        step_length.reshape(blocks, LANES),
        live_mask.reshape(blocks, LANES),
        dest_cell.reshape(blocks, LANES),
    )
    lists = (block_counts, block_lists)

    def shape(*dims):
        return jax.ShapeDtypeStruct(dims, F32)

    x_rows, z_rows, y_rows = packed_rows(fields, CAP_X), packed_rows(fields, CAP_Z), GROUPS * fields
    x_bufs, z_bufs, y_bufs = (
        buffer_shapes("gx", x_rows),
        buffer_shapes("gz", z_rows),
        buffer_shapes("gy", y_rows),
    )

    def x_out(*refs):
        x_out_kernel("gx", fields, *refs)

    out = pl.pallas_call(
        x_out,
        out_shape=x_bufs,
        in_specs=[SMEM] * 2 + [VMEM] * 4,
        out_specs=[VMEM] * len(x_bufs),
        compiler_params=params(8),
        cost_estimate=cost(1 << 16, 1 << 20),
        name="x_out",
    )(*lists, *data)
    x_in = exchange("gx", out)

    def pool_body(*refs):
        pool_kernel(("gx", "gz"), fields, blocks, *refs)

    pool, z_own, z_pick = pl.pallas_call(
        pool_body,
        out_shape=[
            shape(blocks, SLAB, LANES),
            shape(2 * CAP_Z, SLAB, LANES),
            shape(2 * CAP_Z, 16, LANES),
        ],
        in_specs=[SMEM] * 2 + [VMEM] * 4,
        out_specs=[VMEM] * 3,
        compiler_params=params(8),
        cost_estimate=cost(1 << 22, 1 << 20),
        name="pool",
    )(*lists, *data)

    out = pl.pallas_call(
        make_z_out(fields, len(x_in)),
        out_shape=z_bufs,
        in_specs=[VMEM] * (2 + len(x_in)),
        out_specs=[VMEM] * len(z_bufs),
        compiler_params=params(8),
        cost_estimate=cost(1 << 16, 1 << 19),
        name="z_out",
    )(z_own, z_pick, *x_in)
    z_in = exchange("gz", out)

    stay, y_part, z_mask = pl.pallas_call(
        make_bin(fields, blocks, ("gx", "gz", "gy"), len(x_in)),
        out_shape=[shape(*ACC), shape(2, *ACC), shape(3, 16, LANES)],
        in_specs=[SMEM] * 2 + [VMEM] * (1 + len(x_in)),
        out_specs=[VMEM] * 3,
        scratch_shapes=[
            pltpu.SMEM((blocks + 2 * CAP_X + 2 * CAP_Z + 1,), jnp.int32),
            pltpu.VMEM((2 * CAP_X, SLAB, LANES), F32),
            pltpu.VMEM(ACC, F32),
        ],
        compiler_params=params(12),
        cost_estimate=cost(1 << 27, 1 << 20),
        name="bin_held",
    )(*lists, pool, *x_in)

    out = pl.pallas_call(
        make_y_out(fields, len(z_in)),
        out_shape=y_bufs,
        in_specs=[VMEM] * (2 + len(z_in)),
        out_specs=[VMEM] * len(y_bufs),
        compiler_params=params(8),
        cost_estimate=cost(1 << 20, 1 << 19),
        name="y_out",
    )(y_part, z_mask, *z_in)
    y_in = exchange("gy", out)

    stay = pl.pallas_call(
        make_stay(fields, len(z_in)),
        out_shape=shape(y_rows, LANES),
        in_specs=[VMEM] * (2 + len(z_in)),
        out_specs=VMEM,
        compiler_params=params(8),
        cost_estimate=cost(1 << 22, 1 << 19),
        name="bin_z",
    )(stay, z_mask, *z_in)

    return pl.pallas_call(
        make_final(fields, len(y_in)),
        out_shape=shape(fields, CELLS),
        in_specs=[VMEM] * (1 + len(y_in)),
        out_specs=VMEM,
        compiler_params=params(8),
        cost_estimate=cost(1 << 16, 1 << 17),
        name="final",
    )(stay, *y_in)


def solution(mesh):
    axes = ("gx", "gy", "gz")
    placed = (P(None, axes), P(axes), P(axes), P(axes), P(axes, None), P(axes, None))
    return jax.shard_map(
        per_device, mesh=mesh, in_specs=placed, out_specs=P(None, axes), check_vma=False
    )
```

```python
import jax
import jax.numpy as jnp
from jax import lax
from jax.experimental import pallas as pl
from jax.experimental.pallas import tpu as pltpu
from jax.sharding import PartitionSpec as P

CELLS = 512
CAP_X = 6
CAP_Z = 6
CAP_Y = 12
LANES = 128
SLAB = 24
GROUPS = CELLS // LANES
F32 = jnp.float32
BF16 = jnp.bfloat16

VMEM = pl.BlockSpec(memory_space=pltpu.VMEM)
SMEM = pl.BlockSpec(memory_space=pltpu.SMEM)
HBM = pl.BlockSpec(memory_space=pltpu.HBM)
CHUNKS = 4


def params(mib):
    return pltpu.CompilerParams(vmem_limit_bytes=mib << 20)


def cost(flops, nbytes):
    return pl.CostEstimate(flops=flops, bytes_accessed=nbytes, transcendentals=0)


def pairwise(n):
    return n > 2 and n % 2 == 0


def flip_of(axis):
    return lax.axis_index(axis) % 2 if pairwise(lax.axis_size(axis)) else 0


def swapped_of(axis):
    return lax.axis_index(axis) % 2 if pairwise(lax.axis_size(axis)) else 1


def exchange(axis, bufs):
    n = lax.axis_size(axis)
    if n == 2:
        return [lax.ppermute(bufs[0], axis, [(0, 1), (1, 0)])]
    if pairwise(n):
        first = [(i, (i + 1) % n if i % 2 else (i - 1) % n) for i in range(n)]
        second = [(i, (i - 1) % n if i % 2 else (i + 1) % n) for i in range(n)]
    else:
        first = [(i, (i - 1) % n) for i in range(n)]
        second = [(i, (i + 1) % n) for i in range(n)]
    return [lax.ppermute(bufs[0], axis, first), lax.ppermute(bufs[1], axis, second)]


def buffer_shapes(axis, rows):
    n = lax.axis_size(axis)
    one = jax.ShapeDtypeStruct((2 * rows if n == 2 else rows, LANES), F32)
    return [one] if n == 2 else [one, one]


def half(refs, side, rows):
    if len(refs) == 1:
        return refs[0], side * rows
    return refs[side], 0


def packed_rows(fields, count):
    return -(-(count * (fields + 1)) // 8) * 8


def put_block(ref, base, slot, count, fields, slab):
    ref[pl.ds(base + slot * fields, fields), :] = slab[:fields]
    ref[pl.ds(base + count * fields + slot, 1), :] = slab[fields : fields + 1]


def get_block(ref, base, slot, count, fields):
    body = ref[pl.ds(base + slot * fields, fields), :]
    cell = ref[pl.ds(base + count * fields + slot, 1), :]
    pad = jnp.zeros((SLAB - fields - 1, LANES), F32)
    return jnp.concatenate([body, cell, pad], axis=0)


def drifted(fields_ref, step_ref, live_ref, cell_ref, block):
    lanes = pl.ds(pl.multiple_of(block * LANES, LANES), LANES)
    fields = fields_ref.shape[0]
    top = fields_ref[0:8, lanes]
    step = step_ref[pl.ds(block, 1), :]
    live = live_ref[pl.ds(block, 1), :].astype(F32)
    cell = cell_ref[pl.ds(block, 1), :].astype(F32)
    row = lax.broadcasted_iota(jnp.int32, (8, LANES), 0)
    top = top + jnp.where(row < 3, pltpu.roll(top, 5, 0) * step, 0.0)
    rest = fields_ref[8:fields, lanes]
    pad = jnp.zeros((SLAB - fields - 1, LANES), F32)
    return jnp.concatenate([top * live, rest * live, cell, pad], axis=0)


def binned(slabs):
    left, right = [], []
    lane_cell = lax.broadcasted_iota(jnp.int32, (LANES, LANES), 0)
    for slab, field in slabs:
        cell = slab[field : field + 1].astype(jnp.int32)
        low, group = cell & (LANES - 1), cell >> 7
        right.append(jnp.where(lane_cell == low, 1.0, 0.0).astype(BF16))
        high = slab.astype(BF16).astype(F32)
        both = jnp.concatenate([high, slab - high], axis=0)
        left.append(
            jnp.concatenate(
                [jnp.where(group == g, both, 0.0).astype(BF16) for g in range(GROUPS)], axis=0
            )
        )
    return lax.dot_general(
        jnp.concatenate(left, axis=1),
        jnp.concatenate(right, axis=1),
        (((1,), (1,)), ((), ())),
        preferred_element_type=F32,
    )


ACC = (GROUPS * 2 * SLAB, LANES)


def put_sums(ref, base, acc, fields):
    for g in range(GROUPS):
        top = 2 * SLAB * g
        ref[pl.ds(base + g * fields, fields), :] = (
            acc[top : top + fields] + acc[top + SLAB : top + SLAB + fields]
        )


def x_out_kernel(axis, number_hbm, entries_hbm, f_hbm, s_hbm, l_hbm, c_hbm, *refs):
    outs, (f_ref, s_ref, l_ref, c_ref), (number, entries, sems) = refs[:-7], refs[-7:-3], refs[-3:]
    fields, lanes = f_ref.shape
    copies = [
        pltpu.make_async_copy(src, dst, sems.at[i])
        for i, (src, dst) in enumerate(
            ((number_hbm, number), (entries_hbm, entries), (s_hbm, s_ref), (l_hbm, l_ref), (c_hbm, c_ref))
        )
    ]
    part = lanes // CHUNKS
    for i in range(CHUNKS):
        cut = pl.ds(i * part, part)
        copies.append(
            pltpu.make_async_copy(f_hbm.at[:, cut], f_ref.at[:, cut], sems.at[5 + i])
        )
    for copy in copies:
        copy.start()
    for copy in copies:
        copy.wait()
    flip = flip_of(axis)
    rows = packed_rows(fields, CAP_X)
    for side in range(2):
        way = flip if side == 0 else 1 - flip
        ref, base = half(outs, side, rows)
        for j in range(CAP_X):
            entry = entries[0, way * CAP_X + j]
            entry = jnp.where(j < number[0, way], entry, 0)
            slab = drifted(f_ref, s_ref, l_ref, c_ref, entry)
            put_block(ref, base, j, CAP_X, fields, slab * (j < number[0, way]).astype(F32))
        used = CAP_X * (fields + 1)
        if rows > used:
            ref[pl.ds(base + used, rows - used), :] = jnp.zeros((rows - used, LANES), F32)


def arrival_place(entry, first, cap, swapped):
    place = entry - first + cap * swapped
    return jnp.where(place >= 2 * cap, place - 2 * cap, place)


def pool_kernel(axes, fields, blocks, number, entries, f_ref, s_ref, l_ref, c_ref, pool, z_own, z_pick):
    x_axis, z_axis = axes

    @pl.loop(0, blocks, unroll=4)
    def _(b):
        pool[b] = drifted(f_ref, s_ref, l_ref, c_ref, b)

    flip = flip_of(z_axis)
    swapped = swapped_of(x_axis)
    for side in range(2):
        way = flip if side == 0 else 1 - flip
        for j in range(CAP_Z):
            slot = side * CAP_Z + j
            valid = j < number[0, 2 + way]
            entry = entries[0, 2 * CAP_X + way * CAP_Z + j]
            own = valid & (entry < blocks)
            z_own[slot] = pool[jnp.where(own, entry, 0)] * own.astype(F32)
            place = arrival_place(entry, blocks, CAP_X, swapped)
            place = jnp.where(valid & (entry >= blocks), place, -1)
            row = lax.broadcasted_iota(jnp.int32, (16, LANES), 0)
            z_pick[slot] = (row == place).astype(F32)


def make_z_out(fields, n_in):
    x_rows = packed_rows(fields, CAP_X)
    z_rows = packed_rows(fields, CAP_Z)

    def kernel(z_own, z_pick, *refs):
        arrivals, outs = refs[:n_in], refs[n_in:]
        came = []
        for place in range(2 * CAP_X):
            ref, base = half(arrivals, place // CAP_X, x_rows)
            came.append(get_block(ref, base, place % CAP_X, CAP_X, fields))
        for side in range(2):
            ref, base = half(outs, side, z_rows)
            for j in range(CAP_Z):
                slot = side * CAP_Z + j
                slab = z_own[slot]
                for place in range(2 * CAP_X):
                    slab = slab + came[place] * z_pick[slot, place : place + 1, :]
                put_block(ref, base, j, CAP_Z, fields, slab)
            used = CAP_Z * (fields + 1)
            if z_rows > used:
                ref[pl.ds(base + used, z_rows - used), :] = jnp.zeros((z_rows - used, LANES), F32)

    return kernel


def make_bin(fields, blocks, early, axes, n_in):
    x_axis, z_axis, y_axis = axes
    x_rows = packed_rows(fields, CAP_X)
    held = blocks + 2 * CAP_X
    total = held + 2 * CAP_Z

    def kernel(number, entries, pool, *refs):
        arrivals = refs[:n_in]
        stay, y_part, z_mask, own_mask, codes, x_pool, y_acc = refs[n_in:]
        x_swapped, z_swapped, y_flip = swapped_of(x_axis), swapped_of(z_axis), flip_of(y_axis)
        for place in range(2 * CAP_X):
            ref, base = half(arrivals, place // CAP_X, x_rows)
            x_pool[place] = get_block(ref, base, place % CAP_X, CAP_X, fields)

        for b in range(total + 1):
            codes[b] = 0

        def spot(entry):
            in_x = arrival_place(entry, blocks, CAP_X, x_swapped) + blocks
            in_z = arrival_place(entry, held, CAP_Z, z_swapped) + held
            return jnp.where(entry < blocks, entry, jnp.where(entry < held, in_x, in_z))

        at = 0
        for section, cap in enumerate((CAP_X, CAP_Z, CAP_Y)):
            for way in range(2):
                for j in range(cap):
                    valid = j < number[0, 2 * section + way]
                    code = 1 if section < 2 else 2 + (way if isinstance(y_flip, int) else way ^ y_flip)
                    codes[jnp.where(valid, spot(entries[0, at]), total)] = code
                    at += 1

        for b in range(2 * CAP_Z):
            code = codes[held + b]
            for k in range(3):
                wanted = (0, 2, 3)[k]
                z_mask[k, b : b + 1, :] = jnp.full((1, LANES), (code == wanted).astype(F32))

        first = 2 * CAP_X + 2 * CAP_Z
        for side in range(2):
            way = side if isinstance(y_flip, int) else side ^ y_flip

            def one(j):
                entry = spot(entries[0, first + way * CAP_Y + j])
                valid = (j < number[0, 4 + way]) & (entry < held)
                own = valid & (entry < blocks)
                mine = pool[jnp.where(own, entry, 0)] * own.astype(F32)
                theirs = valid & (entry >= blocks)
                return mine + x_pool[jnp.where(theirs, entry - blocks, 0)] * theirs.astype(F32)

            acc = jnp.zeros(ACC, F32)
            for j in range(0, CAP_Y, 4):
                acc = acc + binned([(one(j + i), fields) for i in range(4)])
            y_part[side] = acc

        y_acc[...] = jnp.zeros(ACC, F32)

        for b in range(blocks):
            own_mask[b : b + 1, :] = jnp.full((1, LANES), (codes[b] == 0).astype(F32))

        @pl.loop(0, early // 8)
        def _(step):
            slabs = []
            for i in range(8):
                b = step * 8 + i
                slabs.append((keep_block(pool[b], codes[b] == 0, fields), fields))
            y_acc[...] += binned(slabs)

        acc = y_acc[...]
        for p in range(0, 2 * CAP_X, 6):
            slabs = []
            for i in range(6):
                slabs.append((keep_block(x_pool[p + i], codes[blocks + p + i] == 0, fields), fields))
            acc = acc + binned(slabs)
        stay[...] = acc

    return kernel


def keep_block(slab, keep, fields):
    row = lax.broadcasted_iota(jnp.int32, (SLAB, LANES), 0)
    return slab * jnp.where(row == fields, 1.0, keep.astype(F32))


def z_slab(arrivals, mask, kind, place, rows, fields):
    ref, base = half(arrivals, place // CAP_Z, rows)
    body = ref[pl.ds(base + (place % CAP_Z) * fields, fields), :] * mask[kind, place : place + 1, :]
    cell = ref[pl.ds(base + CAP_Z * fields + place % CAP_Z, 1), :]
    pad = jnp.zeros((SLAB - fields - 1, LANES), F32)
    return jnp.concatenate([body, cell, pad], axis=0)


def make_y_out(fields, n_in):
    rows = packed_rows(fields, CAP_Z)

    def kernel(y_part, z_mask, *refs):
        arrivals, outs = refs[:n_in], refs[n_in:]
        for side in range(2):
            slabs = [
                (z_slab(arrivals, z_mask, 1 + side, place, rows, fields), fields)
                for place in range(2 * CAP_Z)
            ]
            ref, base = half(outs, side, GROUPS * fields)
            put_sums(ref, base, y_part[side] + binned(slabs), fields)

    return kernel


def make_stay(fields, blocks, early, n_in):
    rows = packed_rows(fields, CAP_Z)

    def kernel(stay, z_mask, own_mask, pool, *refs):
        arrivals, out, acc = refs[:n_in], refs[n_in], refs[n_in + 1]
        slabs = [
            (z_slab(arrivals, z_mask, 0, place, rows, fields), fields) for place in range(2 * CAP_Z)
        ]
        acc[...] = stay[...] + binned(slabs)
        row = lax.broadcasted_iota(jnp.int32, (SLAB, LANES), 0)

        @pl.loop(early // 8, blocks // 8)
        def _(step):
            slabs = []
            for i in range(8):
                b = step * 8 + i
                keep = own_mask[pl.ds(b, 1), :]
                slabs.append((pool[b] * jnp.where(row == fields, 1.0, keep), fields))
            acc[...] += binned(slabs)

        put_sums(out, 0, acc[...], fields)

    return kernel


def make_final(fields, n_in):
    def kernel(stay, *refs):
        arrivals, out = refs[:n_in], refs[n_in]
        for g in range(GROUPS):
            total = stay[g * fields : (g + 1) * fields, :]
            for side in range(2):
                ref, base = half(arrivals, side, GROUPS * fields)
                total = total + ref[pl.ds(base + g * fields, fields), :]
            out[:, g * LANES : (g + 1) * LANES] = total

    return kernel


def per_device(particle_fields, step_length, live_mask, dest_cell, block_counts, block_lists):
    fields = particle_fields.shape[0]
    blocks = particle_fields.shape[1] // LANES
    data = (
        particle_fields,
        step_length.reshape(blocks, LANES),
        live_mask.reshape(blocks, LANES),
        dest_cell.reshape(blocks, LANES),
    )
    lists = (block_counts, block_lists)

    def shape(*dims):
        return jax.ShapeDtypeStruct(dims, F32)

    x_rows, z_rows, y_rows = packed_rows(fields, CAP_X), packed_rows(fields, CAP_Z), GROUPS * fields
    x_bufs, z_bufs, y_bufs = (
        buffer_shapes("gx", x_rows),
        buffer_shapes("gz", z_rows),
        buffer_shapes("gy", y_rows),
    )

    def x_out(*refs):
        x_out_kernel("gx", *refs)

    *out, f_in, s_in, l_in, c_in = pl.pallas_call(
        x_out,
        out_shape=x_bufs + [jax.ShapeDtypeStruct(d.shape, d.dtype) for d in data],
        in_specs=[HBM] * 6,
        out_specs=[VMEM] * (len(x_bufs) + 4),
        scratch_shapes=[
            pltpu.SMEM(block_counts.shape, jnp.int32),
            pltpu.SMEM(block_lists.shape, jnp.int32),
            pltpu.SemaphoreType.DMA((5 + CHUNKS,)),
        ],
        compiler_params=params(8),
        cost_estimate=cost(1 << 16, 1 << 20),
        name="x_out",
    )(*(pltpu.with_memory_space_constraint(a, pltpu.HBM) for a in lists + data))
    x_in = exchange("gx", out)

    def pool_body(*refs):
        pool_kernel(("gx", "gz"), fields, blocks, *refs)

    pool, z_own, z_pick = pl.pallas_call(
        pool_body,
        out_shape=[
            shape(blocks, SLAB, LANES),
            shape(2 * CAP_Z, SLAB, LANES),
            shape(2 * CAP_Z, 16, LANES),
        ],
        in_specs=[SMEM] * 2 + [VMEM] * 4,
        out_specs=[VMEM] * 3,
        compiler_params=params(8),
        cost_estimate=cost(1 << 22, 1 << 20),
        name="pool",
    )(*lists, f_in, s_in, l_in, c_in)

    out = pl.pallas_call(
        make_z_out(fields, len(x_in)),
        out_shape=z_bufs,
        in_specs=[VMEM] * (2 + len(x_in)),
        out_specs=[VMEM] * len(z_bufs),
        compiler_params=params(8),
        cost_estimate=cost(1 << 16, 1 << 19),
        name="z_out",
    )(z_own, z_pick, *x_in)
    z_in = exchange("gz", out)

    early = blocks // 32 * 8
    stay, y_part, z_mask, own_mask = pl.pallas_call(
        make_bin(fields, blocks, early, ("gx", "gz", "gy"), len(x_in)),
        out_shape=[shape(*ACC), shape(2, *ACC), shape(3, 16, LANES), shape(blocks, LANES)],
        in_specs=[SMEM] * 2 + [VMEM] * (1 + len(x_in)),
        out_specs=[VMEM] * 4,
        scratch_shapes=[
            pltpu.SMEM((blocks + 2 * CAP_X + 2 * CAP_Z + 1,), jnp.int32),
            pltpu.VMEM((2 * CAP_X, SLAB, LANES), F32),
            pltpu.VMEM(ACC, F32),
        ],
        compiler_params=params(12),
        cost_estimate=cost(1 << 27, 1 << 20),
        name="bin_held",
    )(*lists, pool, *x_in)

    out = pl.pallas_call(
        make_y_out(fields, len(z_in)),
        out_shape=y_bufs,
        in_specs=[VMEM] * (2 + len(z_in)),
        out_specs=[VMEM] * len(y_bufs),
        compiler_params=params(8),
        cost_estimate=cost(1 << 20, 1 << 19),
        name="y_out",
    )(y_part, z_mask, *z_in)
    y_in = exchange("gy", out)

    stay = pl.pallas_call(
        make_stay(fields, blocks, early, len(z_in)),
        out_shape=shape(y_rows, LANES),
        in_specs=[VMEM] * (4 + len(z_in)),
        out_specs=VMEM,
        scratch_shapes=[pltpu.VMEM(ACC, F32)],
        compiler_params=params(8),
        cost_estimate=cost(1 << 26, 1 << 19),
        name="bin_stay",
    )(stay, z_mask, own_mask, pool, *z_in)

    return pl.pallas_call(
        make_final(fields, len(y_in)),
        out_shape=shape(fields, CELLS),
        in_specs=[VMEM] * (1 + len(y_in)),
        out_specs=VMEM,
        compiler_params=params(8),
        cost_estimate=cost(1 << 16, 1 << 17),
        name="final",
    )(stay, *y_in)


def solution(mesh):
    axes = ("gx", "gy", "gz")
    placed = (P(None, axes), P(axes), P(axes), P(axes), P(axes, None), P(axes, None))
    return jax.shard_map(
        per_device, mesh=mesh, in_specs=placed, out_specs=P(None, axes), check_vma=False
    )
```

```python
import jax
import jax.numpy as jnp
from jax import lax
from jax.experimental import pallas as pl
from jax.experimental.pallas import tpu as pltpu
from jax.sharding import PartitionSpec as P

CELLS = 512
CAP_X = 6
CAP_Z = 6
CAP_Y = 12
LANES = 128
SLAB = 24
GROUPS = CELLS // LANES
F32 = jnp.float32
BF16 = jnp.bfloat16

VMEM = pl.BlockSpec(memory_space=pltpu.VMEM)
SMEM = pl.BlockSpec(memory_space=pltpu.SMEM)
HBM = pl.BlockSpec(memory_space=pltpu.HBM)
CHUNKS = 1


def params(mib):
    return pltpu.CompilerParams(vmem_limit_bytes=mib << 20)


def cost(flops, nbytes):
    return pl.CostEstimate(flops=flops, bytes_accessed=nbytes, transcendentals=0)


ORDER = {"gx": "up", "gy": "up", "gz": "down"}


def order_of(axis):
    n = lax.axis_size(axis)
    if n == 2:
        return "down"
    return ORDER[axis] if n % 2 == 0 or ORDER[axis] in ("up", "down") else "down"


def flip_of(axis):
    order = order_of(axis)
    if order in ("up", "down"):
        return int(order == "up")
    parity = lax.axis_index(axis) % 2
    return parity if order == "odd" else 1 - parity


def swapped_of(axis):
    order = order_of(axis)
    return 1 - flip_of(axis) if order in ("up", "down") else flip_of(axis)


def exchange(axis, bufs):
    n = lax.axis_size(axis)
    up, down = [(i, (i + 1) % n) for i in range(n)], [(i, (i - 1) % n) for i in range(n)]
    if n == 2:
        return [lax.ppermute(bufs[0], axis, up)]
    odd = [up[i] if i % 2 else down[i] for i in range(n)]
    even = [down[i] if i % 2 else up[i] for i in range(n)]
    pairs = {"up": (up, down), "down": (down, up), "odd": (odd, even), "even": (even, odd)}
    first, second = pairs[order_of(axis)]
    return [lax.ppermute(bufs[0], axis, first), lax.ppermute(bufs[1], axis, second)]


def buffer_shapes(axis, rows):
    n = lax.axis_size(axis)
    one = jax.ShapeDtypeStruct((2 * rows if n == 2 else rows, LANES), F32)
    return [one] if n == 2 else [one, one]


def half(refs, side, rows):
    if len(refs) == 1:
        return refs[0], side * rows
    return refs[side], 0


def packed_rows(fields, count):
    return -(-(count * (fields + 1)) // 8) * 8


def put_block(ref, base, slot, count, fields, slab):
    ref[pl.ds(base + slot * fields, fields), :] = slab[:fields]
    ref[pl.ds(base + count * fields + slot, 1), :] = slab[fields : fields + 1]


def get_block(ref, base, slot, count, fields):
    body = ref[pl.ds(base + slot * fields, fields), :]
    cell = ref[pl.ds(base + count * fields + slot, 1), :]
    pad = jnp.zeros((SLAB - fields - 1, LANES), F32)
    return jnp.concatenate([body, cell, pad], axis=0)


def drifted(fields_ref, step_ref, live_ref, cell_ref, block):
    lanes = pl.ds(pl.multiple_of(block * LANES, LANES), LANES)
    fields = fields_ref.shape[0]
    top = fields_ref[0:8, lanes]
    step = step_ref[pl.ds(block, 1), :]
    live = live_ref[pl.ds(block, 1), :].astype(F32)
    cell = cell_ref[pl.ds(block, 1), :].astype(F32)
    row = lax.broadcasted_iota(jnp.int32, (8, LANES), 0)
    top = top + jnp.where(row < 3, pltpu.roll(top, 5, 0) * step, 0.0)
    rest = fields_ref[8:fields, lanes]
    pad = jnp.zeros((SLAB - fields - 1, LANES), F32)
    return jnp.concatenate([top * live, rest * live, cell, pad], axis=0)


def binned(slabs):
    left, right = [], []
    lane_cell = lax.broadcasted_iota(jnp.int32, (LANES, LANES), 0)
    for slab, field in slabs:
        cell = slab[field : field + 1].astype(jnp.int32)
        low, group = cell & (LANES - 1), cell >> 7
        right.append(jnp.where(lane_cell == low, 1.0, 0.0).astype(BF16))
        high = slab.astype(BF16).astype(F32)
        both = jnp.concatenate([high, slab - high], axis=0)
        left.append(
            jnp.concatenate(
                [jnp.where(group == g, both, 0.0).astype(BF16) for g in range(GROUPS)], axis=0
            )
        )
    return lax.dot_general(
        jnp.concatenate(left, axis=1),
        jnp.concatenate(right, axis=1),
        (((1,), (1,)), ((), ())),
        preferred_element_type=F32,
    )


ACC = (GROUPS * 2 * SLAB, LANES)


def put_sums(ref, base, acc, fields):
    for g in range(GROUPS):
        top = 2 * SLAB * g
        ref[pl.ds(base + g * fields, fields), :] = (
            acc[top : top + fields] + acc[top + SLAB : top + SLAB + fields]
        )


def x_out_kernel(axis, number_hbm, entries_hbm, f_hbm, s_hbm, l_hbm, c_hbm, *refs):
    outs, (f_ref, s_ref, l_ref, c_ref), (number, entries, sems) = refs[:-7], refs[-7:-3], refs[-3:]
    fields, lanes = f_ref.shape
    copies = [
        pltpu.make_async_copy(src, dst, sems.at[i])
        for i, (src, dst) in enumerate(
            ((number_hbm, number), (entries_hbm, entries), (s_hbm, s_ref), (l_hbm, l_ref), (c_hbm, c_ref))
        )
    ]
    part = lanes // CHUNKS
    for i in range(CHUNKS):
        cut = pl.ds(i * part, part)
        copies.append(
            pltpu.make_async_copy(f_hbm.at[:, cut], f_ref.at[:, cut], sems.at[5 + i])
        )
    for copy in copies:
        copy.start()
    for copy in copies:
        copy.wait()
    flip = flip_of(axis)
    rows = packed_rows(fields, CAP_X)
    for side in range(2):
        way = side ^ flip
        ref, base = half(outs, side, rows)
        for j in range(CAP_X):
            entry = entries[0, way * CAP_X + j]
            entry = jnp.where(j < number[0, way], entry, 0)
            slab = drifted(f_ref, s_ref, l_ref, c_ref, entry)
            put_block(ref, base, j, CAP_X, fields, slab * (j < number[0, way]).astype(F32))
        used = CAP_X * (fields + 1)
        if rows > used:
            ref[pl.ds(base + used, rows - used), :] = jnp.zeros((rows - used, LANES), F32)


def arrival_place(entry, first, cap, swapped):
    place = entry - first + cap * swapped
    return jnp.where(place >= 2 * cap, place - 2 * cap, place)


def pool_kernel(axes, fields, blocks, number, entries, f_ref, s_ref, l_ref, c_ref, pool, z_own, z_pick):
    x_axis, z_axis = axes

    @pl.loop(0, blocks, unroll=4)
    def _(b):
        pool[b] = drifted(f_ref, s_ref, l_ref, c_ref, b)

    flip = flip_of(z_axis)
    swapped = swapped_of(x_axis)
    for side in range(2):
        way = side ^ flip
        for j in range(CAP_Z):
            slot = side * CAP_Z + j
            valid = j < number[0, 2 + way]
            entry = entries[0, 2 * CAP_X + way * CAP_Z + j]
            own = valid & (entry < blocks)
            z_own[slot] = pool[jnp.where(own, entry, 0)] * own.astype(F32)
            place = arrival_place(entry, blocks, CAP_X, swapped)
            place = jnp.where(valid & (entry >= blocks), place, -1)
            row = lax.broadcasted_iota(jnp.int32, (16, LANES), 0)
            z_pick[slot] = (row == place).astype(F32)


def make_z_out(fields, n_in):
    x_rows = packed_rows(fields, CAP_X)
    z_rows = packed_rows(fields, CAP_Z)

    def kernel(z_own, z_pick, *refs):
        arrivals, outs = refs[:n_in], refs[n_in:]
        came = []
        for place in range(2 * CAP_X):
            ref, base = half(arrivals, place // CAP_X, x_rows)
            came.append(get_block(ref, base, place % CAP_X, CAP_X, fields))
        for side in range(2):
            ref, base = half(outs, side, z_rows)
            for j in range(CAP_Z):
                slot = side * CAP_Z + j
                slab = z_own[slot]
                for place in range(2 * CAP_X):
                    slab = slab + came[place] * z_pick[slot, place : place + 1, :]
                put_block(ref, base, j, CAP_Z, fields, slab)
            used = CAP_Z * (fields + 1)
            if z_rows > used:
                ref[pl.ds(base + used, z_rows - used), :] = jnp.zeros((z_rows - used, LANES), F32)

    return kernel


def make_bin(fields, blocks, early, axes, n_in):
    x_axis, z_axis, y_axis = axes
    x_rows = packed_rows(fields, CAP_X)
    held = blocks + 2 * CAP_X
    total = held + 2 * CAP_Z

    def kernel(number, entries, pool, *refs):
        arrivals = refs[:n_in]
        stay, y_part, z_mask, own_mask, codes, x_pool, y_acc = refs[n_in:]
        x_swapped, z_swapped, y_flip = swapped_of(x_axis), swapped_of(z_axis), flip_of(y_axis)
        for place in range(2 * CAP_X):
            ref, base = half(arrivals, place // CAP_X, x_rows)
            x_pool[place] = get_block(ref, base, place % CAP_X, CAP_X, fields)

        for b in range(total + 1):
            codes[b] = 0

        def spot(entry):
            in_x = arrival_place(entry, blocks, CAP_X, x_swapped) + blocks
            in_z = arrival_place(entry, held, CAP_Z, z_swapped) + held
            return jnp.where(entry < blocks, entry, jnp.where(entry < held, in_x, in_z))

        at = 0
        for section, cap in enumerate((CAP_X, CAP_Z, CAP_Y)):
            for way in range(2):
                for j in range(cap):
                    valid = j < number[0, 2 * section + way]
                    code = 1 if section < 2 else 2 + (way ^ y_flip)
                    codes[jnp.where(valid, spot(entries[0, at]), total)] = code
                    at += 1

        for b in range(2 * CAP_Z):
            code = codes[held + b]
            for k in range(3):
                wanted = (0, 2, 3)[k]
                z_mask[k, b : b + 1, :] = jnp.full((1, LANES), (code == wanted).astype(F32))

        first = 2 * CAP_X + 2 * CAP_Z
        for side in range(2):
            way = side ^ y_flip

            def one(j):
                entry = spot(entries[0, first + way * CAP_Y + j])
                valid = (j < number[0, 4 + way]) & (entry < held)
                own = valid & (entry < blocks)
                mine = pool[jnp.where(own, entry, 0)] * own.astype(F32)
                theirs = valid & (entry >= blocks)
                return mine + x_pool[jnp.where(theirs, entry - blocks, 0)] * theirs.astype(F32)

            acc = jnp.zeros(ACC, F32)
            for j in range(0, CAP_Y, 4):
                acc = acc + binned([(one(j + i), fields) for i in range(4)])
            y_part[side] = acc

        y_acc[...] = jnp.zeros(ACC, F32)

        for b in range(blocks):
            own_mask[b : b + 1, :] = jnp.full((1, LANES), (codes[b] == 0).astype(F32))

        @pl.loop(0, early // 8)
        def _(step):
            slabs = []
            for i in range(8):
                b = step * 8 + i
                slabs.append((keep_block(pool[b], codes[b] == 0, fields), fields))
            y_acc[...] += binned(slabs)

        acc = y_acc[...]
        for p in range(0, 2 * CAP_X, 6):
            slabs = []
            for i in range(6):
                slabs.append((keep_block(x_pool[p + i], codes[blocks + p + i] == 0, fields), fields))
            acc = acc + binned(slabs)
        stay[...] = acc

    return kernel


def keep_block(slab, keep, fields):
    row = lax.broadcasted_iota(jnp.int32, (SLAB, LANES), 0)
    return slab * jnp.where(row == fields, 1.0, keep.astype(F32))


def z_slab(arrivals, mask, kind, place, rows, fields):
    ref, base = half(arrivals, place // CAP_Z, rows)
    body = ref[pl.ds(base + (place % CAP_Z) * fields, fields), :] * mask[kind, place : place + 1, :]
    cell = ref[pl.ds(base + CAP_Z * fields + place % CAP_Z, 1), :]
    pad = jnp.zeros((SLAB - fields - 1, LANES), F32)
    return jnp.concatenate([body, cell, pad], axis=0)


def make_y_out(fields, n_in):
    rows = packed_rows(fields, CAP_Z)

    def kernel(y_part, z_mask, *refs):
        arrivals, outs = refs[:n_in], refs[n_in:]
        for side in range(2):
            slabs = [
                (z_slab(arrivals, z_mask, 1 + side, place, rows, fields), fields)
                for place in range(2 * CAP_Z)
            ]
            ref, base = half(outs, side, GROUPS * fields)
            put_sums(ref, base, y_part[side] + binned(slabs), fields)

    return kernel


def make_stay(fields, blocks, early, n_in):
    rows = packed_rows(fields, CAP_Z)

    def kernel(stay, z_mask, own_mask, pool, *refs):
        arrivals, out, acc = refs[:n_in], refs[n_in], refs[n_in + 1]
        slabs = [
            (z_slab(arrivals, z_mask, 0, place, rows, fields), fields) for place in range(2 * CAP_Z)
        ]
        acc[...] = stay[...] + binned(slabs)
        row = lax.broadcasted_iota(jnp.int32, (SLAB, LANES), 0)

        @pl.loop(early // 8, blocks // 8)
        def _(step):
            slabs = []
            for i in range(8):
                b = step * 8 + i
                keep = own_mask[pl.ds(b, 1), :]
                slabs.append((pool[b] * jnp.where(row == fields, 1.0, keep), fields))
            acc[...] += binned(slabs)

        put_sums(out, 0, acc[...], fields)

    return kernel


def make_final(fields, n_in):
    def kernel(stay, *refs):
        arrivals, out = refs[:n_in], refs[n_in]
        for g in range(GROUPS):
            total = stay[g * fields : (g + 1) * fields, :]
            for side in range(2):
                ref, base = half(arrivals, side, GROUPS * fields)
                total = total + ref[pl.ds(base + g * fields, fields), :]
            out[:, g * LANES : (g + 1) * LANES] = total

    return kernel


def per_device(particle_fields, step_length, live_mask, dest_cell, block_counts, block_lists):
    fields = particle_fields.shape[0]
    blocks = particle_fields.shape[1] // LANES
    data = (
        particle_fields,
        step_length.reshape(blocks, LANES),
        live_mask.reshape(blocks, LANES),
        dest_cell.reshape(blocks, LANES),
    )
    lists = (block_counts, block_lists)

    def shape(*dims):
        return jax.ShapeDtypeStruct(dims, F32)

    x_rows, z_rows, y_rows = packed_rows(fields, CAP_X), packed_rows(fields, CAP_Z), GROUPS * fields
    x_bufs, z_bufs, y_bufs = (
        buffer_shapes("gx", x_rows),
        buffer_shapes("gz", z_rows),
        buffer_shapes("gy", y_rows),
    )

    def x_out(*refs):
        x_out_kernel("gx", *refs)

    *out, f_in, s_in, l_in, c_in = pl.pallas_call(
        x_out,
        out_shape=x_bufs + [jax.ShapeDtypeStruct(d.shape, d.dtype) for d in data],
        in_specs=[HBM] * 6,
        out_specs=[VMEM] * (len(x_bufs) + 4),
        scratch_shapes=[
            pltpu.SMEM(block_counts.shape, jnp.int32),
            pltpu.SMEM(block_lists.shape, jnp.int32),
            pltpu.SemaphoreType.DMA((5 + CHUNKS,)),
        ],
        compiler_params=params(8),
        cost_estimate=cost(1 << 16, 1 << 20),
        name="x_out",
    )(*(pltpu.with_memory_space_constraint(a, pltpu.HBM) for a in lists + data))
    x_in = exchange("gx", out)

    def pool_body(*refs):
        pool_kernel(("gx", "gz"), fields, blocks, *refs)

    pool, z_own, z_pick = pl.pallas_call(
        pool_body,
        out_shape=[
            shape(blocks, SLAB, LANES),
            shape(2 * CAP_Z, SLAB, LANES),
            shape(2 * CAP_Z, 16, LANES),
        ],
        in_specs=[SMEM] * 2 + [VMEM] * 4,
        out_specs=[VMEM] * 3,
        compiler_params=params(8),
        cost_estimate=cost(1 << 22, 1 << 20),
        name="pool",
    )(*lists, f_in, s_in, l_in, c_in)

    out = pl.pallas_call(
        make_z_out(fields, len(x_in)),
        out_shape=z_bufs,
        in_specs=[VMEM] * (2 + len(x_in)),
        out_specs=[VMEM] * len(z_bufs),
        compiler_params=params(8),
        cost_estimate=cost(1 << 16, 1 << 19),
        name="z_out",
    )(z_own, z_pick, *x_in)
    z_in = exchange("gz", out)

    early = blocks // 32 * 8
    stay, y_part, z_mask, own_mask = pl.pallas_call(
        make_bin(fields, blocks, early, ("gx", "gz", "gy"), len(x_in)),
        out_shape=[shape(*ACC), shape(2, *ACC), shape(3, 16, LANES), shape(blocks, LANES)],
        in_specs=[SMEM] * 2 + [VMEM] * (1 + len(x_in)),
        out_specs=[VMEM] * 4,
        scratch_shapes=[
            pltpu.SMEM((blocks + 2 * CAP_X + 2 * CAP_Z + 1,), jnp.int32),
            pltpu.VMEM((2 * CAP_X, SLAB, LANES), F32),
            pltpu.VMEM(ACC, F32),
        ],
        compiler_params=params(12),
        cost_estimate=cost(1 << 27, 1 << 20),
        name="bin_held",
    )(*lists, pool, *x_in)

    out = pl.pallas_call(
        make_y_out(fields, len(z_in)),
        out_shape=y_bufs,
        in_specs=[VMEM] * (2 + len(z_in)),
        out_specs=[VMEM] * len(y_bufs),
        compiler_params=params(8),
        cost_estimate=cost(1 << 20, 1 << 19),
        name="y_out",
    )(y_part, z_mask, *z_in)
    y_in = exchange("gy", out)

    stay = pl.pallas_call(
        make_stay(fields, blocks, early, len(z_in)),
        out_shape=shape(y_rows, LANES),
        in_specs=[VMEM] * (4 + len(z_in)),
        out_specs=VMEM,
        scratch_shapes=[pltpu.VMEM(ACC, F32)],
        compiler_params=params(8),
        cost_estimate=cost(1 << 26, 1 << 19),
        name="bin_stay",
    )(stay, z_mask, own_mask, pool, *z_in)

    return pl.pallas_call(
        make_final(fields, len(y_in)),
        out_shape=shape(fields, CELLS),
        in_specs=[VMEM] * (1 + len(y_in)),
        out_specs=VMEM,
        compiler_params=params(8),
        cost_estimate=cost(1 << 16, 1 << 17),
        name="final",
    )(stay, *y_in)


def solution(mesh):
    axes = ("gx", "gy", "gz")
    placed = (P(None, axes), P(axes), P(axes), P(axes), P(axes, None), P(axes, None))
    return jax.shard_map(
        per_device, mesh=mesh, in_specs=placed, out_specs=P(None, axes), check_vma=False
    )
```
